256 devices in a mesh: lat: 64 (over y, x, z_hi), scale: 4 (over z_lo, core).
Axes of the slice: x: 4, y: 4, z: 8 (z_hi: 4, z_lo: 2; z = z_hi * 2 + z_lo), core: 2. Of those that a mesh axis runs over, the one named last changes fastest.
Arguments:
- state: float32 [512, 2, 128, 512], P('lat', None, None, 'scale'), may hold values from -6 to 6
- noise: float32 [512, 2, 128, 512], P('lat', None, None, 'scale'), may hold values from -6 to 6
- slot_wavenumber: int32 [512], replicated, may hold values from 0 to 511, each once
- timescale: float32 [128], replicated, may hold values from 2 to 50
- lengthscale: float32 [128], replicated, may hold values from 128 to 512
Outputs:
- new_state: float32 [512, 2, 128, 512], P('lat', None, None, 'scale')
- pattern: float32 [128, 1536, 3072], P('scale', 'lat')
The draws below stay inside these ranges and needn't reach their ends.
Inputs may be any that keep to these rules, and one draw needn't show every extreme that they name: `slot_wavenumber`: each wavenumber 0 to 511 stands in exactly one slot.
All inputs are finite; a program needn't handle non-finite values.
Results may differ from the reference program's by a relative error of at most 0.0069.
Values may be sent and summed in bfloat16 or wider, within the bound.
No kernel may reach another device: no remote copies, remote signals or barrier semaphores. Data moves between devices by JAX's collectives and lax.ppermute only.
A program may use at most 192 MiB of HBM per device.

```python
import math
import jax
import jax.numpy as jnp
from jax import lax

M = 512
NLAT = 1536
NLON = 3072
FIELDS = 128


def block_scale(key, dims, cuts, low, top_value):
    def one(position, shards_of):
        heights = jax.random.uniform(jax.random.fold_in(jax.random.fold_in(key, 6), position), (shards_of,), jnp.float32, low / len(cuts), top_value / len(cuts))
        return jnp.repeat(jnp.exp(heights), dims[position] // shards_of).reshape((-1,) + (1,) * (len(dims) - position - 1))

    loudness = one(*cuts[0])
    for cut in cuts[1:]:
        loudness = loudness * one(*cut)
    return loudness


def gaussian(own_key, extent, spread, most, shards=(), kind=jnp.bfloat16):
    level = block_scale(own_key, extent, shards, -0.22, 0.18) if shards else 1.0
    result = jax.random.normal(own_key, extent, jnp.float32) * spread * level
    return jnp.minimum(jnp.maximum(result, -most), most).astype(kind)


def setup_inputs(seed: int = 0) -> dict:
    streams_of = jax.random.split(jax.random.key(seed), 6)
    return {
        "state": gaussian(streams_of[0], (M, 2, FIELDS, M), 1.0, 6.0, ((0, 64), (3, 4)), jnp.float32),
        "noise": gaussian(streams_of[1], (M, 2, FIELDS, M), 1.0, 6.0, ((0, 64), (3, 4)), jnp.float32),
        "slot_wavenumber": jax.random.permutation(streams_of[2], M).astype(jnp.int32),
        "timescale": jnp.clip(jnp.exp(jax.random.uniform(streams_of[3], (FIELDS,), jnp.float32, math.log(2.0), math.log(50.0))), 2.0, 50.0),
        "lengthscale": jnp.clip(jnp.exp(jax.random.uniform(streams_of[4], (FIELDS,), jnp.float32, math.log(128.0), math.log(512.0))), 128.0, 512.0),
    }


log_floor = -60.0

def start_values(orders_local, sine_row):
    orders = orders_local.astype(jnp.float32)[:, None]
    log_head = 0.5 * (jax.scipy.special.gammaln(2.0 * orders + 1.0) + jnp.log(2.0 * orders + 1.0) - math.log(2.0)) - orders * math.log(2.0) - jax.scipy.special.gammaln(orders + 1.0)
    log_start = log_head + orders * jnp.log(sine_row)[None, :]
    return jnp.where(log_start >= log_floor, jnp.exp(jnp.maximum(log_start, log_floor)), 0.0)

def ratio(degree, orders):
    squared = degree * degree
    return jnp.sqrt(jnp.maximum(squared - orders * orders, 0.0) / (4.0 * squared - 1.0))

def next_row(degree, orders, cosine_row, pole_start, previous, earlier):
    ratio_here = ratio(degree, orders)
    ratio_before = ratio(degree - 1.0, orders)
    is_above = degree > orders
    grown_row = (cosine_row * previous - ratio_before * earlier) / jnp.where(is_above, ratio_here, 1.0)
    return jnp.where(degree == orders, pole_start, jnp.where(is_above, grown_row, 0.0))

def fourier_table(slot_wavenumber):
    points = jnp.arange(NLON).astype(jnp.int32)
    phase_index = slot_wavenumber[:, None] * points[None, :] % NLON
    angles = phase_index.astype(jnp.float32) * (2.0 * math.pi / NLON)
    weight = jnp.where(slot_wavenumber == 0, 1.0, 2.0) / M
    fourier = jnp.stack([weight[:, None] * jnp.cos(angles), -weight[:, None] * jnp.sin(angles)], axis=1)
    return fourier.astype(jnp.bfloat16)

def reference(state, noise, slot_wavenumber, timescale, lengthscale):
    decay_rate = jnp.exp(-1.0 / timescale)
    degrees = jnp.arange(M).astype(jnp.float32)
    amplitude = jnp.sqrt(1.0 - decay_rate * decay_rate)[:, None] * jnp.exp(-degrees[None, :] * (degrees[None, :] + 1.0) / (2.0 * lengthscale[:, None] ** 2)) * (M / lengthscale)[:, None]
    new_state = decay_rate[None, None, :, None] * state + amplitude[None, None] * noise
    spectra = new_state.astype(jnp.bfloat16)
    colatitude = (jnp.arange(NLAT).astype(jnp.float32) + 0.5) * (math.pi / NLAT)
    cosine_row = jnp.cos(colatitude)[None, :]
    sine_row = jnp.sin(colatitude)
    block_width = min(M, 64)

    def block(block_index):
        first_slot = (block_index * block_width).astype(jnp.int32)
        orders_local = lax.dynamic_slice_in_dim(slot_wavenumber, first_slot, block_width)
        block_coeff = lax.dynamic_slice_in_dim(spectra, first_slot, block_width, 0)
        orders = orders_local.astype(jnp.float32)[:, None]
        pole_start = start_values(orders_local, sine_row)
        zeros_row = jnp.zeros((block_width, NLAT), jnp.float32)

        def advance(recurrence, degree):
            previous, earlier = recurrence
            new_row = next_row(degree, orders, cosine_row, pole_start, previous, earlier)
            return ((new_row, previous), new_row)
        _, legendre = lax.scan(advance, (zeros_row, zeros_row), jnp.arange(M).astype(jnp.float32))
        legendre = legendre.astype(jnp.bfloat16)
        product = jnp.einsum('srfn,nsl->srfl', block_coeff.astype(jnp.float32), legendre.astype(jnp.float32))
        return product.astype(jnp.bfloat16)
    grid_spec = lax.map(block, jnp.arange(M // block_width).astype(jnp.int32))
    grid_spec = grid_spec.reshape(M, 2, FIELDS, NLAT)
    fourier = fourier_table(slot_wavenumber)
    pattern = jnp.einsum('srfl,srk->flk', grid_spec.astype(jnp.float32), fourier.astype(jnp.float32))
    return (new_state, pattern)
```

```python
import math

import jax
import jax.numpy as jnp
import numpy as np
from jax import lax
from jax.experimental import pallas as pl
from jax.experimental.pallas import tpu as pltpu
from jax.sharding import PartitionSpec as P

M = 512
NLAT = 1536
NLON = 3072
FIELDS = 128
HALF = NLAT // 2
LANES = 128
LAT_PARTS = 64
SCALE_PARTS = 4
SLOTS = M // LAT_PARTS
ROWS = NLAT // LAT_PARTS
OWN_FIELDS = FIELDS // SCALE_PARTS
PAIRS = SLOTS // 2
CHUNK = 128
WIDTH = 512

log_floor = -60.0


def vmem_params(*semantics):
    return pltpu.CompilerParams(
        dimension_semantics=semantics, vmem_limit_bytes=56 * 1024 * 1024
    )


def latitude_constants():
    colatitude = (np.arange(HALF) + 0.5) * (math.pi / NLAT)
    cosine = np.cos(colatitude)
    log_sine = np.log(np.sin(colatitude))
    return np.stack([cosine, log_sine]).astype(np.float32)


def log_head_table():
    lgamma = np.vectorize(math.lgamma)
    order = np.arange(M, dtype=np.float64)
    head = (
        0.5 * (lgamma(2.0 * order + 1.0) + np.log(2.0 * order + 1.0) - math.log(2.0))
        - order * math.log(2.0)
        - lgamma(order + 1.0)
    )
    return head.astype(np.float32)[None]


def update_kernel(where_ref, scales_ref, state_ref, noise_ref, new_ref, spectra_ref, factor):
    @pl.when(pl.program_id(0) == 0)
    def _():
        time_row = jnp.broadcast_to(scales_ref[0:1, :], (FIELDS, FIELDS))
        length_row = jnp.broadcast_to(scales_ref[1:2, :], (FIELDS, FIELDS))
        timescale = time_row.T
        lengthscale = length_row.T
        decay = jnp.exp(-1.0 / timescale)
        first = where_ref[1] * CHUNK
        degree = (first + lax.broadcasted_iota(jnp.int32, (FIELDS, CHUNK), 1)).astype(jnp.float32)
        factor[0] = decay
        factor[1] = (
            jnp.sqrt(1.0 - decay * decay)
            * jnp.exp(-degree * (degree + 1.0) / (2.0 * (lengthscale * lengthscale)))
            * (M / lengthscale)
        )

    for part in range(2):
        new = factor[0] * state_ref[0, part] + factor[1] * noise_ref[0, part]
        new_ref[0, part] = new
        rounded = new.astype(jnp.bfloat16)
        for owner in range(SCALE_PARTS):
            spectra_ref[owner, 0, part] = rounded[owner * OWN_FIELDS : (owner + 1) * OWN_FIELDS]


def update(where, scales, state, noise):
    block = pl.BlockSpec((1, 2, FIELDS, CHUNK), lambda s: (s, 0, 0, 0))
    return pl.pallas_call(
        update_kernel,
        grid=(SLOTS,),
        in_specs=[
            pl.BlockSpec(memory_space=pltpu.SMEM),
            pl.BlockSpec((2, FIELDS), lambda s: (0, 0)),
            block,
            block,
        ],
        out_specs=[
            block,
            pl.BlockSpec((SCALE_PARTS, 1, 2, OWN_FIELDS, CHUNK), lambda s: (0, s, 0, 0, 0)),
        ],
        out_shape=[
            jax.ShapeDtypeStruct((SLOTS, 2, FIELDS, CHUNK), jnp.float32),
            jax.ShapeDtypeStruct((SCALE_PARTS, SLOTS, 2, OWN_FIELDS, CHUNK), jnp.bfloat16),
        ],
        scratch_shapes=[pltpu.VMEM((2, FIELDS, CHUNK), jnp.float32)],
        compiler_params=vmem_params("arbitrary"),
        name="update",
    )(where, scales, state, noise)


def own_orders(where_ref, orders_ref, shape):
    slot = lax.broadcasted_iota(jnp.int32, shape, 0)
    orders = jnp.zeros(shape, jnp.int32)
    for s in range(SLOTS):
        orders = jnp.where(slot == s, orders_ref[where_ref[0] * SLOTS + s], orders)
    return orders


def ratio_at(degree, orders):
    squared = degree * degree
    return jnp.sqrt(jnp.maximum(squared - orders * orders, 0.0) / (4.0 * squared - 1.0))


def table_kernel(where_ref, orders_ref, lats_ref, head_ref, table_ref, rows, carried, pole):
    step = pl.program_id(0)
    order_tile = own_orders(where_ref, orders_ref, (SLOTS, LANES))
    order_real = order_tile.astype(jnp.float32)

    @pl.when(step == 0)
    def _():
        wide = own_orders(where_ref, orders_ref, (SLOTS, M))
        chosen = lax.broadcasted_iota(jnp.int32, (SLOTS, M), 1) == wide
        head = jnp.sum(jnp.where(chosen, head_ref[...], 0.0), axis=1, keepdims=True)
        log_start = head + order_real[:, :1] * lats_ref[1:2, :]
        pole[...] = jnp.where(
            log_start >= log_floor, jnp.exp(jnp.maximum(log_start, log_floor)), 0.0
        )
        carried[...] = jnp.zeros_like(carried)

    degree = (step * CHUNK + lax.broadcasted_iota(jnp.int32, (SLOTS, LANES), 1)).astype(jnp.float32)
    above = degree > order_real
    here = jnp.where(above, ratio_at(degree, order_real), 1.0)
    gain = jnp.where(above, 1.0 / here, 0.0)
    loss = jnp.where(above, ratio_at(degree - 1.0, order_real) / here, 0.0)
    cosine = jnp.broadcast_to(lats_ref[0:1, :], (SLOTS, HALF))
    start = pole[...]
    previous = carried[0]
    earlier = carried[1]
    for i in range(CHUNK):
        begins = order_tile[:, :1] == step * CHUNK + i
        new = gain[:, i : i + 1] * (cosine * previous) - loss[:, i : i + 1] * earlier
        new = jnp.where(begins, start, new)
        for tile in range(HALF // LANES):
            rows[tile, i * SLOTS : (i + 1) * SLOTS, :] = new[:, tile * LANES : (tile + 1) * LANES]
        previous, earlier = (new, previous)
    carried[0] = previous
    carried[1] = earlier
    for s in range(SLOTS):
        for tile in range(HALF // LANES):
            table_ref[s, :, tile * LANES : (tile + 1) * LANES] = rows[
                tile, pl.ds(s, CHUNK, stride=SLOTS), :
            ].astype(jnp.bfloat16)


def legendre_table(where, orders, lats, head):
    return pl.pallas_call(
        table_kernel,
        grid=(M // CHUNK,),
        in_specs=[
            pl.BlockSpec(memory_space=pltpu.SMEM),
            pl.BlockSpec(memory_space=pltpu.SMEM),
            pl.BlockSpec((2, HALF), lambda i: (0, 0)),
            pl.BlockSpec((1, M), lambda i: (0, 0)),
        ],
        out_specs=pl.BlockSpec((SLOTS, CHUNK, HALF), lambda i: (0, i, 0)),
        out_shape=jax.ShapeDtypeStruct((SLOTS, M, HALF), jnp.bfloat16),
        scratch_shapes=[
            pltpu.VMEM((HALF // LANES, CHUNK * SLOTS, LANES), jnp.float32),
            pltpu.VMEM((2, SLOTS, HALF), jnp.float32),
            pltpu.VMEM((SLOTS, HALF), jnp.float32),
        ],
        compiler_params=vmem_params("arbitrary"),
        name="legendre",
    )(where, orders, lats, head)


def project_kernel(where_ref, orders_ref, spectra_ref, table_ref, out_ref):
    pair = pl.program_id(0)
    north = []
    south = []
    lane = lax.broadcasted_iota(jnp.int32, (1, CHUNK), 1)
    for half in range(2):
        order = orders_ref[where_ref[0] * SLOTS + 2 * pair + half]
        sign = (1 - 2 * ((lane + order) % 2)).astype(jnp.float32).astype(jnp.bfloat16)
        blocks = [
            spectra_ref[b, half].reshape(2 * OWN_FIELDS, CHUNK) for b in range(SCALE_PARTS)
        ]
        left = jnp.concatenate(
            [jnp.concatenate([b, b * sign], axis=0) for b in blocks], axis=1
        )
        product = jnp.dot(left, table_ref[half], preferred_element_type=jnp.float32)
        north.append(product[: 2 * OWN_FIELDS])
        south.append(product[2 * OWN_FIELDS :])
    upper = jnp.concatenate(north, axis=0).T.reshape(LAT_PARTS // 2, ROWS, LANES)
    lower = jnp.concatenate(south, axis=0).T.reshape(LAT_PARTS // 2, ROWS, LANES)
    upper = upper.astype(jnp.bfloat16)
    lower = lower.astype(jnp.bfloat16)
    for d in range(LAT_PARTS // 2):
        out_ref[d, 0] = upper[d]
        out_ref[LAT_PARTS - 1 - d, 0] = lower[d]


def project(where, orders, spectra, table):
    return pl.pallas_call(
        project_kernel,
        grid=(PAIRS,),
        in_specs=[
            pl.BlockSpec(memory_space=pltpu.SMEM),
            pl.BlockSpec(memory_space=pltpu.SMEM),
            pl.BlockSpec(
                (SCALE_PARTS, 2, 2, OWN_FIELDS, CHUNK), lambda p: (0, p, 0, 0, 0)
            ),
            pl.BlockSpec((2, M, HALF), lambda p: (p, 0, 0)),
        ],
        out_specs=pl.BlockSpec((LAT_PARTS, 1, ROWS, LANES), lambda p: (0, p, 0, 0)),
        out_shape=jax.ShapeDtypeStruct((LAT_PARTS, PAIRS, ROWS, LANES), jnp.bfloat16),
        compiler_params=vmem_params("arbitrary"),
        name="project",
    )(where, orders, spectra, table)


def fourier_table(slot_wavenumber):
    orders = slot_wavenumber.reshape(LAT_PARTS, 2, 2, 2).transpose(1, 3, 2, 0)
    orders = orders.reshape(2, 2, 1, 2 * LAT_PARTS)
    orders = jnp.broadcast_to(orders, (2, 2, 2, 2 * LAT_PARTS)).reshape(2 * M, 1)
    row = lax.broadcasted_iota(jnp.int32, (2 * M, 1), 0)
    quarter = (row // (2 * LAT_PARTS)) % 2 * (NLON // 4)
    points = lax.broadcasted_iota(jnp.int32, (1, NLON), 1)
    phase_index = (orders * points + quarter) % NLON
    angles = phase_index.astype(jnp.float32) * (2.0 * math.pi / NLON)
    weight = jnp.where(orders == 0, 1.0, 2.0) / M
    return (weight * jnp.cos(angles)).astype(jnp.bfloat16)


def synthesis_kernel(where_ref, grid_ref, fourier_ref, out_ref, wide, turned, left):
    @pl.when(pl.program_id(0) == 0)
    def _():
        wide[...] = grid_ref[...].astype(jnp.float32).reshape(wide.shape)
        is_south = where_ref[0] >= LAT_PARTS // 2
        for row in range(ROWS):
            target = jnp.where(is_south, ROWS - 1 - row, row)
            for group in range(2):
                stacked = jnp.concatenate(
                    [
                        wide[pl.ds((2 * group + t) * ROWS + row, LAT_PARTS, stride=PAIRS * ROWS), :]
                        for t in range(2)
                    ],
                    axis=0,
                ).T
                for q in range(4):
                    turned[4 * group + q, pl.ds(target, OWN_FIELDS, stride=ROWS), :] = stacked[
                        q * OWN_FIELDS : (q + 1) * OWN_FIELDS
                    ]
        for q in range(8):
            left[:, q * LANES : (q + 1) * LANES] = turned[q].astype(jnp.bfloat16)

    product = jnp.dot(left[...], fourier_ref[...], preferred_element_type=jnp.float32)
    out_ref[...] = product.reshape(out_ref.shape)


def synthesize(where, grid_spec, fourier):
    return pl.pallas_call(
        synthesis_kernel,
        grid=(NLON // WIDTH,),
        in_specs=[
            pl.BlockSpec(memory_space=pltpu.SMEM),
            pl.BlockSpec((LAT_PARTS, PAIRS, ROWS, LANES), lambda k: (0, 0, 0, 0)),
            pl.BlockSpec((2 * M, WIDTH), lambda k: (0, k)),
        ],
        out_specs=pl.BlockSpec((OWN_FIELDS, ROWS, WIDTH), lambda k: (0, 0, k)),
        out_shape=jax.ShapeDtypeStruct((OWN_FIELDS, ROWS, NLON), jnp.float32),
        scratch_shapes=[
            pltpu.VMEM((LAT_PARTS * PAIRS * ROWS, LANES), jnp.float32),
            pltpu.VMEM((8, OWN_FIELDS * ROWS, LANES), jnp.float32),
            pltpu.VMEM((OWN_FIELDS * ROWS, 2 * M), jnp.bfloat16),
        ],
        compiler_params=vmem_params("arbitrary"),
        name="synthesis",
    )(where, grid_spec, fourier)


def exchanged(spectra):
    return lax.all_to_all(spectra, "scale", 0, 0, tiled=True)


def on_device(state, noise, slot_wavenumber, timescale, lengthscale):
    where = jnp.stack([lax.axis_index("lat"), lax.axis_index("scale")])
    scales = jnp.stack([timescale, lengthscale])
    lats = jnp.asarray(latitude_constants())
    head = jnp.asarray(log_head_table())
    new_state, spectra = update(where, scales, state, noise)
    spectra = exchanged(spectra)
    table = legendre_table(where, slot_wavenumber, lats, head)
    grid_spec = project(where, slot_wavenumber, spectra, table)
    grid_spec = lax.all_to_all(grid_spec, "lat", 0, 0, tiled=True)
    pattern = synthesize(where, grid_spec, fourier_table(slot_wavenumber))
    return (new_state, pattern)


def solution(mesh):
    placed = (P("lat", None, None, "scale"), P("lat", None, None, "scale"), P(), P(), P())
    return jax.shard_map(
        on_device,
        mesh=mesh,
        in_specs=placed,
        out_specs=(P("lat", None, None, "scale"), P("scale", "lat", None)),
        check_vma=False,
    )
```

```python
import math

import jax
import jax.numpy as jnp
import numpy as np
from jax import lax
from jax.experimental import pallas as pl
from jax.experimental.pallas import tpu as pltpu
from jax.sharding import PartitionSpec as P

M = 512
NLAT = 1536
NLON = 3072
FIELDS = 128
HALF = NLAT // 2
LANES = 128
LAT_PARTS = 64
SCALE_PARTS = 4
SLOTS = M // LAT_PARTS
ROWS = NLAT // LAT_PARTS
OWN_FIELDS = FIELDS // SCALE_PARTS
PAIRS = SLOTS // 2
CHUNK = 128
GROUP = 2
WIDTH = 512

log_floor = -60.0


def vmem_params(*semantics):
    return pltpu.CompilerParams(
        dimension_semantics=semantics, vmem_limit_bytes=56 * 1024 * 1024
    )


def latitude_constants():
    colatitude = (np.arange(HALF) + 0.5) * (math.pi / NLAT)
    cosine = np.cos(colatitude)
    log_sine = np.log(np.sin(colatitude))
    return np.stack([cosine, log_sine]).astype(np.float32)


def log_head_table():
    lgamma = np.vectorize(math.lgamma)
    order = np.arange(M, dtype=np.float64)
    head = (
        0.5 * (lgamma(2.0 * order + 1.0) + np.log(2.0 * order + 1.0) - math.log(2.0))
        - order * math.log(2.0)
        - lgamma(order + 1.0)
    )
    return head.astype(np.float32)[None]


def update_kernel(time_ref, length_ref, state_ref, noise_ref, new_ref, spectra_ref, factor):
    @pl.when(pl.program_id(0) == 0)
    def _():
        timescale = jnp.broadcast_to(time_ref[...], (FIELDS, FIELDS)).T
        lengthscale = jnp.broadcast_to(length_ref[...], (FIELDS, FIELDS)).T
        decay = jnp.exp(-1.0 / timescale)
        first = lax.axis_index("scale") * CHUNK
        degree = (first + lax.broadcasted_iota(jnp.int32, (FIELDS, CHUNK), 1)).astype(jnp.float32)
        factor[0] = decay
        factor[1] = (
            jnp.sqrt(1.0 - decay * decay)
            * jnp.exp(-degree * (degree + 1.0) / (2.0 * (lengthscale * lengthscale)))
            * (M / lengthscale)
        )

    for slot in range(GROUP):
        for part in range(2):
            new = factor[0] * state_ref[slot, part] + factor[1] * noise_ref[slot, part]
            new_ref[slot, part] = new
            rounded = new.astype(jnp.bfloat16)
            for owner in range(SCALE_PARTS):
                spectra_ref[owner, slot, part] = rounded[
                    owner * OWN_FIELDS : (owner + 1) * OWN_FIELDS
                ]


def update(timescale, lengthscale, state, noise):
    block = pl.BlockSpec((GROUP, 2, FIELDS, CHUNK), lambda s: (s, 0, 0, 0))
    line = pl.BlockSpec((1, FIELDS), lambda s: (0, 0))
    return pl.pallas_call(
        update_kernel,
        grid=(SLOTS // GROUP,),
        in_specs=[line, line, block, block],
        out_specs=[
            block,
            pl.BlockSpec((SCALE_PARTS, GROUP, 2, OWN_FIELDS, CHUNK), lambda s: (0, s, 0, 0, 0)),
        ],
        out_shape=[
            jax.ShapeDtypeStruct((SLOTS, 2, FIELDS, CHUNK), jnp.float32),
            jax.ShapeDtypeStruct((SCALE_PARTS, SLOTS, 2, OWN_FIELDS, CHUNK), jnp.bfloat16),
        ],
        scratch_shapes=[pltpu.VMEM((2, FIELDS, CHUNK), jnp.float32)],
        compiler_params=vmem_params("arbitrary"),
        name="update",
    )(timescale, lengthscale, state, noise)


def own_orders(orders_ref, shape):
    slot = lax.broadcasted_iota(jnp.int32, shape, 0)
    orders = jnp.zeros(shape, jnp.int32)
    for s in range(SLOTS):
        orders = jnp.where(slot == s, orders_ref[lax.axis_index("lat") * SLOTS + s], orders)
    return orders


def ratio_at(degree, orders):
    squared = degree * degree
    return jnp.sqrt(jnp.maximum(squared - orders * orders, 0.0) / (4.0 * squared - 1.0))


def table_kernel(orders_ref, lats_ref, head_ref, table_ref, rows, carried, pole):
    step = pl.program_id(0)
    order_tile = own_orders(orders_ref, (SLOTS, LANES))
    order_real = order_tile.astype(jnp.float32)

    @pl.when(step == 0)
    def _():
        wide = own_orders(orders_ref, (SLOTS, M))
        chosen = lax.broadcasted_iota(jnp.int32, (SLOTS, M), 1) == wide
        head = jnp.sum(jnp.where(chosen, head_ref[...], 0.0), axis=1, keepdims=True)
        log_start = head + order_real[:, :1] * lats_ref[1:2, :]
        pole[...] = jnp.where(
            log_start >= log_floor, jnp.exp(jnp.maximum(log_start, log_floor)), 0.0
        )
        carried[...] = jnp.zeros_like(carried)

    degree = (step * CHUNK + lax.broadcasted_iota(jnp.int32, (SLOTS, LANES), 1)).astype(jnp.float32)
    above = degree > order_real
    here = jnp.where(above, ratio_at(degree, order_real), 1.0)
    gain = jnp.where(above, 1.0 / here, 0.0)
    loss = jnp.where(above, ratio_at(degree - 1.0, order_real) / here, 0.0)
    cosine = jnp.broadcast_to(lats_ref[0:1, :], (SLOTS, HALF))
    start = pole[...]
    previous = carried[0]
    earlier = carried[1]
    for i in range(CHUNK):
        begins = order_tile[:, :1] == step * CHUNK + i
        new = gain[:, i : i + 1] * (cosine * previous) - loss[:, i : i + 1] * earlier
        new = jnp.where(begins, start, new)
        for tile in range(HALF // LANES):
            rows[tile, i * SLOTS : (i + 1) * SLOTS, :] = new[:, tile * LANES : (tile + 1) * LANES]
        previous, earlier = (new, previous)
    carried[0] = previous
    carried[1] = earlier
    for s in range(SLOTS):
        for tile in range(HALF // LANES):
            table_ref[s, :, tile * LANES : (tile + 1) * LANES] = rows[
                tile, pl.ds(s, CHUNK, stride=SLOTS), :
            ].astype(jnp.bfloat16)


def legendre_table(orders, lats, head):
    return pl.pallas_call(
        table_kernel,
        grid=(M // CHUNK,),
        in_specs=[
            pl.BlockSpec(memory_space=pltpu.SMEM),
            pl.BlockSpec((2, HALF), lambda i: (0, 0)),
            pl.BlockSpec((1, M), lambda i: (0, 0)),
        ],
        out_specs=pl.BlockSpec((SLOTS, CHUNK, HALF), lambda i: (0, i, 0)),
        out_shape=jax.ShapeDtypeStruct((SLOTS, M, HALF), jnp.bfloat16),
        scratch_shapes=[
            pltpu.VMEM((HALF // LANES, CHUNK * SLOTS, LANES), jnp.float32),
            pltpu.VMEM((2, SLOTS, HALF), jnp.float32),
            pltpu.VMEM((SLOTS, HALF), jnp.float32),
        ],
        compiler_params=vmem_params("arbitrary"),
        name="legendre",
    )(orders, lats, head)


def project_kernel(orders_ref, spectra_ref, table_ref, out_ref):
    pair = pl.program_id(0)
    north = []
    south = []
    lane = lax.broadcasted_iota(jnp.int32, (1, CHUNK), 1)
    for half in range(2):
        order = orders_ref[lax.axis_index("lat") * SLOTS + 2 * pair + half]
        sign = (1 - 2 * ((lane + order) % 2)).astype(jnp.float32).astype(jnp.bfloat16)
        blocks = [
            spectra_ref[b, 2 * pair + half].reshape(2 * OWN_FIELDS, CHUNK) for b in range(SCALE_PARTS)
        ]
        left = jnp.concatenate(
            [jnp.concatenate([b, b * sign], axis=0) for b in blocks], axis=1
        )
        product = jnp.dot(left, table_ref[half], preferred_element_type=jnp.float32)
        north.append(product[: 2 * OWN_FIELDS])
        south.append(product[2 * OWN_FIELDS :])
    upper = jnp.concatenate(north, axis=0).T.reshape(LAT_PARTS // 2, ROWS, LANES)
    lower = jnp.concatenate(south, axis=0).T.reshape(LAT_PARTS // 2, ROWS, LANES)
    upper = upper.astype(jnp.bfloat16)
    lower = lower.astype(jnp.bfloat16)
    for d in range(LAT_PARTS // 2):
        out_ref[d, 0] = upper[d]
        out_ref[LAT_PARTS - 1 - d, 0] = lower[d]


def project(orders, spectra, table):
    return pl.pallas_call(
        project_kernel,
        grid=(PAIRS,),
        in_specs=[
            pl.BlockSpec(memory_space=pltpu.SMEM),
            pl.BlockSpec(memory_space=pltpu.VMEM),
            pl.BlockSpec((2, M, HALF), lambda p: (p, 0, 0)),
        ],
        out_specs=pl.BlockSpec((LAT_PARTS, 1, ROWS, LANES), lambda p: (0, p, 0, 0)),
        out_shape=jax.ShapeDtypeStruct((LAT_PARTS, PAIRS, ROWS, LANES), jnp.bfloat16),
        compiler_params=vmem_params("arbitrary"),
        name="project",
    )(orders, spectra, table)


def remainder(value, divisor):
    return value - divisor * jnp.floor(value * (1.0 / divisor))


def fourier_kernel(orders_ref, table_ref):
    order = jnp.broadcast_to(orders_ref[0], (LANES, LANES)).T
    lane = lax.broadcasted_iota(jnp.int32, (LANES, LANES), 1).astype(jnp.float32)
    weight = jnp.where(order == 0.0, 1.0, 2.0) / M
    fine = remainder(order * lane, float(NLON)) * (2.0 * math.pi / NLON)
    coarse = remainder(order * lane, float(NLON // LANES)) * (2.0 * math.pi * LANES / NLON)
    fine_cos = jnp.cos(fine)
    fine_sin = jnp.sin(fine)
    coarse_cos = weight * jnp.cos(coarse)
    coarse_sin = weight * jnp.sin(coarse)
    for a in range(NLON // LANES):
        cos_a = coarse_cos[:, a : a + 1]
        sin_a = coarse_sin[:, a : a + 1]
        lanes = slice(a * LANES, (a + 1) * LANES)
        table_ref[:LANES, lanes] = (cos_a * fine_cos - sin_a * fine_sin).astype(jnp.bfloat16)
        table_ref[LANES:, lanes] = (-sin_a * fine_cos - cos_a * fine_sin).astype(jnp.bfloat16)


def fourier_table(slot_wavenumber):
    orders = slot_wavenumber.reshape(LAT_PARTS, 2, 2, 2).transpose(1, 3, 2, 0)
    orders = orders.reshape(4, 1, 2 * LAT_PARTS).astype(jnp.float32)
    return pl.pallas_call(
        fourier_kernel,
        grid=(4,),
        in_specs=[pl.BlockSpec((1, 1, LANES), lambda i: (i, 0, 0))],
        out_specs=pl.BlockSpec((2 * LANES, NLON), lambda i: (i, 0)),
        out_shape=jax.ShapeDtypeStruct((2 * M, NLON), jnp.bfloat16),
        compiler_params=vmem_params("arbitrary"),
        name="fourier",
    )(orders)


def synthesis_kernel(grid_ref, fourier_ref, out_ref, wide, turned, left):
    @pl.when(pl.program_id(0) == 0)
    def _():
        wide[...] = grid_ref[...].astype(jnp.float32).reshape(wide.shape)
        is_south = lax.axis_index("lat") >= LAT_PARTS // 2
        for row in range(ROWS):
            target = jnp.where(is_south, ROWS - 1 - row, row)
            for group in range(2):
                stacked = jnp.concatenate(
                    [
                        wide[pl.ds((2 * group + t) * ROWS + row, LAT_PARTS, stride=PAIRS * ROWS), :]
                        for t in range(2)
                    ],
                    axis=0,
                ).T
                for q in range(4):
                    turned[4 * group + q, pl.ds(target, OWN_FIELDS, stride=ROWS), :] = stacked[
                        q * OWN_FIELDS : (q + 1) * OWN_FIELDS
                    ]
        for q in range(8):
            left[:, q * LANES : (q + 1) * LANES] = turned[q].astype(jnp.bfloat16)

    product = jnp.dot(left[...], fourier_ref[...], preferred_element_type=jnp.float32)
    out_ref[...] = product.reshape(out_ref.shape)


def synthesize(grid_spec, fourier):
    return pl.pallas_call(
        synthesis_kernel,
        grid=(NLON // WIDTH,),
        in_specs=[
            pl.BlockSpec(memory_space=pltpu.VMEM),
            pl.BlockSpec((2 * M, WIDTH), lambda k: (0, k)),
        ],
        out_specs=pl.BlockSpec((OWN_FIELDS, ROWS, WIDTH), lambda k: (0, 0, k)),
        out_shape=jax.ShapeDtypeStruct((OWN_FIELDS, ROWS, NLON), jnp.float32),
        scratch_shapes=[
            pltpu.VMEM((LAT_PARTS * PAIRS * ROWS, LANES), jnp.float32),
            pltpu.VMEM((8, OWN_FIELDS * ROWS, LANES), jnp.float32),
            pltpu.VMEM((OWN_FIELDS * ROWS, 2 * M), jnp.bfloat16),
        ],
        compiler_params=vmem_params("arbitrary"),
        name="synthesis",
    )(grid_spec, fourier)


def exchanged(spectra):
    return lax.all_to_all(spectra, "scale", 0, 0, tiled=True)


def on_device(state, noise, slot_wavenumber, timescale, lengthscale):
    lats = jnp.asarray(latitude_constants())
    head = jnp.asarray(log_head_table())
    new_state, spectra = update(timescale[None], lengthscale[None], state, noise)
    spectra = exchanged(spectra)
    table = legendre_table(slot_wavenumber, lats, head)
    grid_spec = project(slot_wavenumber, spectra, table)
    grid_spec = lax.all_to_all(grid_spec, "lat", 0, 0, tiled=True)
    pattern = synthesize(grid_spec, fourier_table(slot_wavenumber))
    return (new_state, pattern)


def solution(mesh):
    placed = (P("lat", None, None, "scale"), P("lat", None, None, "scale"), P(), P(), P())
    return jax.shard_map(
        on_device,
        mesh=mesh,
        in_specs=placed,
        out_specs=(P("lat", None, None, "scale"), P("scale", "lat", None)),
        check_vma=False,
    )
```

```python
import functools
import math

import jax
import jax.numpy as jnp
import numpy as np
from jax import lax
from jax.experimental import pallas as pl
from jax.experimental.pallas import tpu as pltpu
from jax.sharding import PartitionSpec as P

M = 512
NLAT = 1536
NLON = 3072
FIELDS = 128
HALF = NLAT // 2
LANES = 128
LAT_PARTS = 64
SCALE_PARTS = 4
SLOTS = M // LAT_PARTS
ROWS = NLAT // LAT_PARTS
OWN_FIELDS = FIELDS // SCALE_PARTS
PAIRS = SLOTS // 2
CHUNK = 128
GROUP = 2
WIDTH = 512
PITCH = PAIRS * ROWS + 8
BANDS = ((0, 8), (8, 16))

log_floor = -60.0


whole = pl.BlockSpec(memory_space=pltpu.VMEM)
outside = pl.BlockSpec(memory_space=pltpu.HBM)


def vmem_params(mebibytes, **others):
    return pltpu.CompilerParams(vmem_limit_bytes=mebibytes * 1024 * 1024, **others)


def latitude_constants():
    colatitude = (np.arange(HALF) + 0.5) * (math.pi / NLAT)
    cosine = np.cos(colatitude)
    log_sine = np.log(np.sin(colatitude))
    return np.stack([cosine, log_sine]).astype(np.float32)


def log_head_table():
    lgamma = np.vectorize(math.lgamma)
    order = np.arange(M, dtype=np.float64)
    head = (
        0.5 * (lgamma(2.0 * order + 1.0) + np.log(2.0 * order + 1.0) - math.log(2.0))
        - order * math.log(2.0)
        - lgamma(order + 1.0)
    )
    return head.astype(np.float32)[None]


def update_kernel(time_ref, length_ref, state_ref, noise_ref, new_ref, spectra_ref, factor):
    @pl.when(pl.program_id(0) == 0)
    def _():
        timescale = jnp.broadcast_to(time_ref[...], (FIELDS, FIELDS)).T
        lengthscale = jnp.broadcast_to(length_ref[...], (FIELDS, FIELDS)).T
        decay = jnp.exp(-1.0 / timescale)
        first = lax.axis_index("scale") * CHUNK
        degree = (first + lax.broadcasted_iota(jnp.int32, (FIELDS, CHUNK), 1)).astype(jnp.float32)
        factor[0] = decay
        factor[1] = (
            jnp.sqrt(1.0 - decay * decay)
            * jnp.exp(-degree * (degree + 1.0) / (2.0 * (lengthscale * lengthscale)))
            * (M / lengthscale)
        )

    for slot in range(GROUP):
        for part in range(2):
            new = factor[0] * state_ref[slot, part] + factor[1] * noise_ref[slot, part]
            new_ref[slot, part] = new
            rounded = new.astype(jnp.bfloat16)
            for owner in range(SCALE_PARTS):
                spectra_ref[owner, slot, part] = rounded[
                    owner * OWN_FIELDS : (owner + 1) * OWN_FIELDS
                ]


def update(timescale, lengthscale, state, noise):
    block = pl.BlockSpec((GROUP, 2, FIELDS, CHUNK), lambda s: (s, 0, 0, 0))
    line = pl.BlockSpec((1, FIELDS), lambda s: (0, 0))
    return pl.pallas_call(
        update_kernel,
        grid=(SLOTS // GROUP,),
        in_specs=[line, line, block, block],
        out_specs=[
            block,
            pl.BlockSpec((SCALE_PARTS, GROUP, 2, OWN_FIELDS, CHUNK), lambda s: (0, s, 0, 0, 0)),
        ],
        out_shape=[
            jax.ShapeDtypeStruct((SLOTS, 2, FIELDS, CHUNK), jnp.float32),
            jax.ShapeDtypeStruct((SCALE_PARTS, SLOTS, 2, OWN_FIELDS, CHUNK), jnp.bfloat16),
        ],
        scratch_shapes=[pltpu.VMEM((2, FIELDS, CHUNK), jnp.float32)],
        compiler_params=vmem_params(58, dimension_semantics=("arbitrary",)),
        name="update",
    )(timescale, lengthscale, state, noise)


def own_orders(orders_ref, shape):
    slot = lax.broadcasted_iota(jnp.int32, shape, 0)
    orders = jnp.zeros(shape, jnp.int32)
    for s in range(SLOTS):
        orders = jnp.where(slot == s, orders_ref[lax.axis_index("lat") * SLOTS + s], orders)
    return orders


def ratio_at(degree, orders):
    squared = degree * degree
    return jnp.sqrt(jnp.maximum(squared - orders * orders, 0.0) / (4.0 * squared - 1.0))


def table_kernel(orders_ref, lats_ref, head_ref, table_ref, rows, carried, pole):
    step = pl.program_id(0)
    order_tile = own_orders(orders_ref, (SLOTS, LANES))
    order_real = order_tile.astype(jnp.float32)

    @pl.when(step == 0)
    def _():
        wide = own_orders(orders_ref, (SLOTS, M))
        chosen = lax.broadcasted_iota(jnp.int32, (SLOTS, M), 1) == wide
        head = jnp.sum(jnp.where(chosen, head_ref[...], 0.0), axis=1, keepdims=True)
        log_start = head + order_real[:, :1] * lats_ref[1:2, :]
        pole[...] = jnp.where(
            log_start >= log_floor, jnp.exp(jnp.maximum(log_start, log_floor)), 0.0
        )
        carried[...] = jnp.zeros_like(carried)

    degree = (step * CHUNK + lax.broadcasted_iota(jnp.int32, (SLOTS, LANES), 1)).astype(jnp.float32)
    above = degree > order_real
    here = jnp.where(above, ratio_at(degree, order_real), 1.0)
    gain = jnp.where(above, 1.0 / here, 0.0)
    loss = jnp.where(above, ratio_at(degree - 1.0, order_real) / here, 0.0)
    cosine = jnp.broadcast_to(lats_ref[0:1, :], (SLOTS, HALF))
    start = pole[...]
    previous = carried[0]
    earlier = carried[1]
    for i in range(CHUNK):
        begins = order_tile[:, :1] == step * CHUNK + i
        new = gain[:, i : i + 1] * (cosine * previous) - loss[:, i : i + 1] * earlier
        new = jnp.where(begins, start, new)
        for tile in range(HALF // LANES):
            rows[tile, i * SLOTS : (i + 1) * SLOTS, :] = new[:, tile * LANES : (tile + 1) * LANES]
        previous, earlier = (new, previous)
    carried[0] = previous
    carried[1] = earlier
    for s in range(SLOTS):
        for tile in range(HALF // LANES):
            table_ref[s, :, tile * LANES : (tile + 1) * LANES] = rows[
                tile, pl.ds(s, CHUNK, stride=SLOTS), :
            ].astype(jnp.bfloat16)


def legendre_table(orders, lats, head):
    return pl.pallas_call(
        table_kernel,
        grid=(M // CHUNK,),
        in_specs=[
            pl.BlockSpec(memory_space=pltpu.SMEM),
            pl.BlockSpec((2, HALF), lambda i: (0, 0)),
            pl.BlockSpec((1, M), lambda i: (0, 0)),
        ],
        out_specs=pl.BlockSpec((SLOTS, CHUNK, HALF), lambda i: (0, i, 0)),
        out_shape=jax.ShapeDtypeStruct((SLOTS, M, HALF), jnp.bfloat16),
        scratch_shapes=[
            pltpu.VMEM((HALF // LANES, CHUNK * SLOTS, LANES), jnp.float32),
            pltpu.VMEM((2, SLOTS, HALF), jnp.float32),
            pltpu.VMEM((SLOTS, HALF), jnp.float32),
        ],
        compiler_params=vmem_params(58, dimension_semantics=("arbitrary",)),
        name="legendre",
    )(orders, lats, head)


def project_kernel(orders_ref, spectra_ref, table_ref, out_ref, table, arrived):
    lane = lax.broadcasted_iota(jnp.int32, (1, CHUNK), 1)
    copies = [
        pltpu.make_async_copy(table_ref.at[s], table.at[s], arrived.at[s]) for s in range(SLOTS)
    ]
    for copy in copies:
        copy.start()
    for pair in range(PAIRS):
        north = []
        south = []
        for half in range(2):
            order = orders_ref[lax.axis_index("lat") * SLOTS + 2 * pair + half]
            sign = (1 - 2 * ((lane + order) % 2)).astype(jnp.float32).astype(jnp.bfloat16)
            blocks = [
                spectra_ref[b, 2 * pair + half].reshape(2 * OWN_FIELDS, CHUNK)
                for b in range(SCALE_PARTS)
            ]
            left = jnp.concatenate(
                [jnp.concatenate([b, b * sign], axis=0) for b in blocks], axis=1
            )
            copies[2 * pair + half].wait()
            product = jnp.dot(left, table[2 * pair + half], preferred_element_type=jnp.float32)
            north.append(product[: 2 * OWN_FIELDS])
            south.append(product[2 * OWN_FIELDS :])
        upper = jnp.concatenate(north, axis=0).T.reshape(LAT_PARTS // 2, ROWS, LANES)
        lower = jnp.concatenate(south, axis=0).T.reshape(LAT_PARTS // 2, ROWS, LANES)
        upper = upper.astype(jnp.bfloat16)
        lower = lower.astype(jnp.bfloat16)
        for d in range(LAT_PARTS // 2):
            out_ref[d, pair] = upper[d]
            out_ref[LAT_PARTS - 1 - d, pair] = lower[d]


def project(orders, spectra, table):
    return pl.pallas_call(
        project_kernel,
        in_specs=[pl.BlockSpec(memory_space=pltpu.SMEM), whole, outside],
        out_specs=whole,
        out_shape=jax.ShapeDtypeStruct((LAT_PARTS, PAIRS, ROWS, LANES), jnp.bfloat16),
        scratch_shapes=[
            pltpu.VMEM((SLOTS, M, HALF), jnp.bfloat16),
            pltpu.SemaphoreType.DMA((SLOTS,)),
        ],
        compiler_params=vmem_params(52),
        name="project",
    )(orders, spectra, table)


def remainder(value, divisor):
    return value - divisor * jnp.floor(value * (1.0 / divisor))


def fourier_kernel(orders_ref, table_ref):
    order = jnp.broadcast_to(orders_ref[0], (LANES, LANES)).T
    lane = lax.broadcasted_iota(jnp.int32, (LANES, LANES), 1).astype(jnp.float32)
    weight = jnp.where(order == 0.0, 1.0, 2.0) / M
    fine = remainder(order * lane, float(NLON)) * (2.0 * math.pi / NLON)
    coarse = remainder(order * lane, float(NLON // LANES)) * (2.0 * math.pi * LANES / NLON)
    fine_cos = jnp.cos(fine)
    fine_sin = jnp.sin(fine)
    coarse_cos = weight * jnp.cos(coarse)
    coarse_sin = weight * jnp.sin(coarse)
    for a in range(NLON // LANES):
        cos_a = coarse_cos[:, a : a + 1]
        sin_a = coarse_sin[:, a : a + 1]
        lanes = slice(a * LANES, (a + 1) * LANES)
        table_ref[:LANES, lanes] = (cos_a * fine_cos - sin_a * fine_sin).astype(jnp.bfloat16)
        table_ref[LANES:, lanes] = (-sin_a * fine_cos - cos_a * fine_sin).astype(jnp.bfloat16)


def fourier_table(slot_wavenumber):
    orders = slot_wavenumber.reshape(LAT_PARTS, 2, 2, 2).transpose(1, 3, 2, 0)
    orders = orders.reshape(4, 1, 2 * LAT_PARTS).astype(jnp.float32)
    return pl.pallas_call(
        fourier_kernel,
        grid=(4,),
        in_specs=[pl.BlockSpec((1, 1, LANES), lambda i: (i, 0, 0))],
        out_specs=pl.BlockSpec((2 * LANES, NLON), lambda i: (i, 0)),
        out_shape=jax.ShapeDtypeStruct((2 * M, NLON), jnp.bfloat16),
        compiler_params=vmem_params(58, dimension_semantics=("arbitrary",)),
        name="fourier",
    )(orders)


def synthesis_kernel(
    grid_ref, fourier_ref, out_ref, wide, turned, left, done, fourier, arrived, fetched
):
    fetches = []
    for k in range(NLON // WIDTH):
        points = slice(k * WIDTH, (k + 1) * WIDTH)
        fetches.append(
            pltpu.make_async_copy(
                fourier_ref.at[:, points], fourier.at[:, points], fetched.at[k]
            )
        )
        fetches[k].start()
    for source in range(LAT_PARTS):
        wide[source * PITCH : source * PITCH + PAIRS * ROWS, :] = (
            grid_ref[source].astype(jnp.float32).reshape(PAIRS * ROWS, LANES)
        )
    is_south = lax.axis_index("lat") >= LAT_PARTS // 2

    def transpose(first, count, row, group):
        source_row = jnp.where(is_south, ROWS - 1 - (first + row), first + row)
        stacked = jnp.concatenate(
            [
                wide[pl.ds((2 * group + t) * ROWS + source_row, LAT_PARTS, stride=PITCH), :]
                for t in range(2)
            ],
            axis=0,
        ).T
        for q in range(4):
            turned[
                4 * group + q, pl.ds(OWN_FIELDS * first + row, OWN_FIELDS, stride=count), :
            ] = stacked[q * OWN_FIELDS : (q + 1) * OWN_FIELDS]

    def narrow(first, count, q):
        rows = slice(OWN_FIELDS * first, OWN_FIELDS * (first + count))
        left[rows, q * LANES : (q + 1) * LANES] = turned[q, rows, :].astype(jnp.bfloat16)

    def preparation(first, count):
        steps = []
        for group in range(2):
            steps += [
                functools.partial(transpose, first, count, row, group) for row in range(count)
            ]
            steps += [functools.partial(narrow, first, count, 4 * group + q) for q in range(4)]
        return steps

    copies = []
    for step in preparation(*BANDS[0]):
        step()
    for band, (first, count) in enumerate(BANDS):
        rows = slice(OWN_FIELDS * first, OWN_FIELDS * (first + count))
        pending = preparation(*BANDS[band + 1]) if band + 1 < len(BANDS) else []
        share = -(-len(pending) // (NLON // WIDTH))
        for k in range(NLON // WIDTH):
            points = slice(k * WIDTH, (k + 1) * WIDTH)
            if band == 0:
                fetches[k].wait()
            product = jnp.dot(left[rows, :], fourier[:, points], preferred_element_type=jnp.float32)
            done[:, first : first + count, points] = product.reshape(OWN_FIELDS, count, WIDTH)
            copy = pltpu.make_async_copy(
                done.at[:, first : first + count, points],
                out_ref.at[:, first : first + count, points],
                arrived.at[len(copies)],
            )
            copy.start()
            copies.append(copy)
            for step in pending[k * share : (k + 1) * share]:
                step()
    for copy in copies:
        copy.wait()


def synthesize(grid_spec, fourier):
    return pl.pallas_call(
        synthesis_kernel,
        in_specs=[whole, outside],
        out_specs=outside,
        out_shape=jax.ShapeDtypeStruct((OWN_FIELDS, ROWS, NLON), jnp.float32),
        scratch_shapes=[
            pltpu.VMEM((LAT_PARTS * PITCH, LANES), jnp.float32),
            pltpu.VMEM((8, OWN_FIELDS * ROWS, LANES), jnp.float32),
            pltpu.VMEM((OWN_FIELDS * ROWS, 2 * M), jnp.bfloat16),
            pltpu.VMEM((OWN_FIELDS, ROWS, NLON), jnp.float32),
            pltpu.VMEM((2 * M, NLON), jnp.bfloat16),
            pltpu.SemaphoreType.DMA((len(BANDS) * (NLON // WIDTH),)),
            pltpu.SemaphoreType.DMA((NLON // WIDTH,)),
        ],
        compiler_params=vmem_params(52),
        name="synthesis",
    )(grid_spec, fourier)


def exchanged(spectra):
    return lax.all_to_all(spectra, "scale", 0, 0, tiled=True)


def on_device(state, noise, slot_wavenumber, timescale, lengthscale):
    lats = jnp.asarray(latitude_constants())
    head = jnp.asarray(log_head_table())
    new_state, spectra = update(timescale[None], lengthscale[None], state, noise)
    spectra = exchanged(spectra)
    table = legendre_table(slot_wavenumber, lats, head)
    grid_spec = project(slot_wavenumber, spectra, table)
    grid_spec = lax.all_to_all(grid_spec, "lat", 0, 0, tiled=True)
    pattern = synthesize(grid_spec, fourier_table(slot_wavenumber))
    return (new_state, pattern)


def solution(mesh):
    placed = (P("lat", None, None, "scale"), P("lat", None, None, "scale"), P(), P(), P())
    return jax.shard_map(
        on_device,
        mesh=mesh,
        in_specs=placed,
        out_specs=(P("lat", None, None, "scale"), P("scale", "lat", None)),
        check_vma=False,
    )
```

```python
import functools
import math

import jax
import jax.numpy as jnp
import numpy as np
from jax import lax
from jax.experimental import pallas as pl
from jax.experimental.pallas import tpu as pltpu
from jax.sharding import PartitionSpec as P

M = 512
NLAT = 1536
NLON = 3072
FIELDS = 128
HALF = NLAT // 2
LANES = 128
LAT_PARTS = 64
SCALE_PARTS = 4
SLOTS = M // LAT_PARTS
ROWS = NLAT // LAT_PARTS
OWN_FIELDS = FIELDS // SCALE_PARTS
PAIRS = SLOTS // 2
CHUNK = 128
GROUP = 4
WIDTH = 512
PITCH = PAIRS * ROWS + 8
BANDS = ((0, 8), (8, 8), (16, 8))

log_floor = -60.0


whole = pl.BlockSpec(memory_space=pltpu.VMEM)
outside = pl.BlockSpec(memory_space=pltpu.HBM)


def vmem_params(mebibytes, **others):
    return pltpu.CompilerParams(vmem_limit_bytes=mebibytes * 1024 * 1024, **others)


def latitude_constants():
    colatitude = (np.arange(HALF) + 0.5) * (math.pi / NLAT)
    cosine = np.cos(colatitude)
    log_sine = np.log(np.sin(colatitude))
    return np.stack([cosine, log_sine]).astype(np.float32)


def log_head_table():
    lgamma = np.vectorize(math.lgamma)
    order = np.arange(M, dtype=np.float64)
    head = (
        0.5 * (lgamma(2.0 * order + 1.0) + np.log(2.0 * order + 1.0) - math.log(2.0))
        - order * math.log(2.0)
        - lgamma(order + 1.0)
    )
    return head.astype(np.float32)[None]


def partner(scale, offset):
    low = scale % 2
    high = scale // 2
    return (high + offset // 2) % 2 * 2 + (low + offset) % 2


def update_kernel(time_ref, length_ref, state_ref, noise_ref, new_ref, *rest):
    spectra_refs = rest[:SCALE_PARTS]
    factor = rest[SCALE_PARTS]
    @pl.when(pl.program_id(0) == 0)
    def _():
        timescale = jnp.broadcast_to(time_ref[...], (FIELDS, FIELDS)).T
        lengthscale = jnp.broadcast_to(length_ref[...], (FIELDS, FIELDS)).T
        decay = jnp.exp(-1.0 / timescale)
        first = lax.axis_index("scale") * CHUNK
        degree = (first + lax.broadcasted_iota(jnp.int32, (FIELDS, CHUNK), 1)).astype(jnp.float32)
        factor[0] = decay
        factor[1] = (
            jnp.sqrt(1.0 - decay * decay)
            * jnp.exp(-degree * (degree + 1.0) / (2.0 * (lengthscale * lengthscale)))
            * (M / lengthscale)
        )

    for slot in range(GROUP):
        for part in range(2):
            new = factor[0] * state_ref[slot, part] + factor[1] * noise_ref[slot, part]
            new_ref[slot, part] = new
            for offset in range(SCALE_PARTS):
                owner = partner(lax.axis_index("scale"), offset)
                first = pl.multiple_of(owner * OWN_FIELDS, OWN_FIELDS)
                spectra_refs[offset][slot, part] = new_ref[
                    slot, part, pl.ds(first, OWN_FIELDS), :
                ].astype(jnp.bfloat16)


def update(timescale, lengthscale, state, noise):
    block = pl.BlockSpec((GROUP, 2, FIELDS, CHUNK), lambda s: (s, 0, 0, 0))
    line = pl.BlockSpec((1, FIELDS), lambda s: (0, 0))
    return pl.pallas_call(
        update_kernel,
        grid=(SLOTS // GROUP,),
        in_specs=[line, line, block, block],
        out_specs=[block]
        + [pl.BlockSpec((GROUP, 2, OWN_FIELDS, CHUNK), lambda s: (s, 0, 0, 0))] * SCALE_PARTS,
        out_shape=[jax.ShapeDtypeStruct((SLOTS, 2, FIELDS, CHUNK), jnp.float32)]
        + [jax.ShapeDtypeStruct((SLOTS, 2, OWN_FIELDS, CHUNK), jnp.bfloat16)] * SCALE_PARTS,
        scratch_shapes=[pltpu.VMEM((2, FIELDS, CHUNK), jnp.float32)],
        compiler_params=vmem_params(58, dimension_semantics=("arbitrary",)),
        name="update",
    )(timescale, lengthscale, state, noise)


def own_orders(orders_ref, shape):
    slot = lax.broadcasted_iota(jnp.int32, shape, 0)
    orders = jnp.zeros(shape, jnp.int32)
    for s in range(SLOTS):
        orders = jnp.where(slot == s, orders_ref[lax.axis_index("lat") * SLOTS + s], orders)
    return orders


def ratio_at(degree, orders):
    squared = degree * degree
    return jnp.sqrt(jnp.maximum(squared - orders * orders, 0.0) / (4.0 * squared - 1.0))


def table_kernel(orders_ref, lats_ref, head_ref, table_ref, rows, carried, pole):
    step = pl.program_id(0)
    order_tile = own_orders(orders_ref, (SLOTS, LANES))
    order_real = order_tile.astype(jnp.float32)

    @pl.when(step == 0)
    def _():
        wide = own_orders(orders_ref, (SLOTS, M))
        chosen = lax.broadcasted_iota(jnp.int32, (SLOTS, M), 1) == wide
        head = jnp.sum(jnp.where(chosen, head_ref[...], 0.0), axis=1, keepdims=True)
        log_start = head + order_real[:, :1] * lats_ref[1:2, :]
        pole[...] = jnp.where(
            log_start >= log_floor, jnp.exp(jnp.maximum(log_start, log_floor)), 0.0
        )
        carried[...] = jnp.zeros_like(carried)

    degree = (step * CHUNK + lax.broadcasted_iota(jnp.int32, (SLOTS, LANES), 1)).astype(jnp.float32)
    above = degree > order_real
    here = jnp.where(above, ratio_at(degree, order_real), 1.0)
    gain = jnp.where(above, 1.0 / here, 0.0)
    loss = jnp.where(above, ratio_at(degree - 1.0, order_real) / here, 0.0)
    cosine = jnp.broadcast_to(lats_ref[0:1, :], (SLOTS, HALF))
    start = pole[...]
    previous = carried[0]
    earlier = carried[1]
    for i in range(CHUNK):
        begins = order_tile[:, :1] == step * CHUNK + i
        new = gain[:, i : i + 1] * (cosine * previous) - loss[:, i : i + 1] * earlier
        new = jnp.where(begins, start, new)
        for tile in range(HALF // LANES):
            rows[tile, i * SLOTS : (i + 1) * SLOTS, :] = new[:, tile * LANES : (tile + 1) * LANES]
        previous, earlier = (new, previous)
    carried[0] = previous
    carried[1] = earlier
    for s in range(SLOTS):
        for tile in range(HALF // LANES):
            table_ref[s, :, tile * LANES : (tile + 1) * LANES] = rows[
                tile, pl.ds(s, CHUNK, stride=SLOTS), :
            ].astype(jnp.bfloat16)


def legendre_table(orders, lats, head):
    return pl.pallas_call(
        table_kernel,
        grid=(M // CHUNK,),
        in_specs=[
            pl.BlockSpec(memory_space=pltpu.SMEM),
            pl.BlockSpec((2, HALF), lambda i: (0, 0)),
            pl.BlockSpec((1, M), lambda i: (0, 0)),
        ],
        out_specs=pl.BlockSpec((SLOTS, CHUNK, HALF), lambda i: (0, i, 0)),
        out_shape=jax.ShapeDtypeStruct((SLOTS, M, HALF), jnp.bfloat16),
        scratch_shapes=[
            pltpu.VMEM((HALF // LANES, CHUNK * SLOTS, LANES), jnp.float32),
            pltpu.VMEM((2, SLOTS, HALF), jnp.float32),
            pltpu.VMEM((SLOTS, HALF), jnp.float32),
        ],
        compiler_params=vmem_params(58, dimension_semantics=("arbitrary",)),
        name="legendre",
    )(orders, lats, head)


def project_kernel(orders_ref, *rest):
    spectra_refs = rest[:SCALE_PARTS]
    table_ref, out_ref, table, arrived = rest[SCALE_PARTS:]
    lane = lax.broadcasted_iota(jnp.int32, (1, CHUNK), 1)
    copies = []
    for s in range(SLOTS):
        for b in range(SCALE_PARTS):
            block = partner(lax.axis_index("scale"), b)
            first = pl.multiple_of(block * CHUNK, CHUNK)
            copies.append(
                pltpu.make_async_copy(
                    table_ref.at[s, pl.ds(first, CHUNK)],
                    table.at[s, pl.ds(b * CHUNK, CHUNK)],
                    arrived.at[s, b],
                )
            )
            copies[-1].start()
    for pair in range(PAIRS):
        north = []
        south = []
        for half in range(2):
            order = orders_ref[lax.axis_index("lat") * SLOTS + 2 * pair + half]
            sign = (1 - 2 * ((lane + order) % 2)).astype(jnp.float32).astype(jnp.bfloat16)
            blocks = [
                spectra_refs[b][2 * pair + half].reshape(2 * OWN_FIELDS, CHUNK)
                for b in range(SCALE_PARTS)
            ]
            left = jnp.concatenate(
                [jnp.concatenate([b, b * sign], axis=0) for b in blocks], axis=1
            )
            slot = 2 * pair + half
            for copy in copies[slot * SCALE_PARTS : (slot + 1) * SCALE_PARTS]:
                copy.wait()
            product = jnp.dot(left, table[2 * pair + half], preferred_element_type=jnp.float32)
            north.append(product[: 2 * OWN_FIELDS])
            south.append(product[2 * OWN_FIELDS :])
        upper = jnp.concatenate(north, axis=0).T.reshape(LAT_PARTS // 2, ROWS, LANES)
        lower = jnp.concatenate(south, axis=0).T.reshape(LAT_PARTS // 2, ROWS, LANES)
        upper = upper.astype(jnp.bfloat16)
        lower = lower.astype(jnp.bfloat16)
        for d in range(LAT_PARTS // 2):
            out_ref[d, pair] = upper[d]
            out_ref[LAT_PARTS - 1 - d, pair] = lower[d]


def project(orders, spectra, table):
    return pl.pallas_call(
        project_kernel,
        in_specs=[pl.BlockSpec(memory_space=pltpu.SMEM)] + [whole] * SCALE_PARTS + [outside],
        out_specs=whole,
        out_shape=jax.ShapeDtypeStruct((LAT_PARTS, PAIRS, ROWS, LANES), jnp.bfloat16),
        scratch_shapes=[
            pltpu.VMEM((SLOTS, M, HALF), jnp.bfloat16),
            pltpu.SemaphoreType.DMA((SLOTS, SCALE_PARTS)),
        ],
        compiler_params=vmem_params(52),
        name="project",
    )(orders, *spectra, table)


def remainder(value, divisor):
    return value - divisor * jnp.floor(value * (1.0 / divisor))


def fourier_kernel(orders_ref, table_ref):
    order = jnp.broadcast_to(orders_ref[0], (LANES, LANES)).T
    lane = lax.broadcasted_iota(jnp.int32, (LANES, LANES), 1).astype(jnp.float32)
    weight = jnp.where(order == 0.0, 1.0, 2.0) / M
    fine = remainder(order * lane, float(NLON)) * (2.0 * math.pi / NLON)
    coarse = remainder(order * lane, float(NLON // LANES)) * (2.0 * math.pi * LANES / NLON)
    fine_cos = jnp.cos(fine)
    fine_sin = jnp.sin(fine)
    coarse_cos = weight * jnp.cos(coarse)
    coarse_sin = weight * jnp.sin(coarse)
    for a in range(NLON // LANES):
        cos_a = coarse_cos[:, a : a + 1]
        sin_a = coarse_sin[:, a : a + 1]
        lanes = slice(a * LANES, (a + 1) * LANES)
        table_ref[:LANES, lanes] = (cos_a * fine_cos - sin_a * fine_sin).astype(jnp.bfloat16)
        table_ref[LANES:, lanes] = (-sin_a * fine_cos - cos_a * fine_sin).astype(jnp.bfloat16)


def fourier_table(slot_wavenumber):
    orders = slot_wavenumber.reshape(LAT_PARTS, 2, 2, 2).transpose(1, 3, 2, 0)
    orders = orders.reshape(4, 1, 2 * LAT_PARTS).astype(jnp.float32)
    return pl.pallas_call(
        fourier_kernel,
        grid=(4,),
        in_specs=[pl.BlockSpec((1, 1, LANES), lambda i: (i, 0, 0))],
        out_specs=pl.BlockSpec((2 * LANES, NLON), lambda i: (i, 0)),
        out_shape=jax.ShapeDtypeStruct((2 * M, NLON), jnp.bfloat16),
        compiler_params=vmem_params(58, dimension_semantics=("arbitrary",)),
        name="fourier",
    )(orders)


def synthesis_kernel(
    grid_ref, fourier_ref, out_ref, wide, turned, left, done, fourier, arrived, fetched
):
    fetches = []
    for k in range(NLON // WIDTH):
        points = slice(k * WIDTH, (k + 1) * WIDTH)
        fetches.append(
            pltpu.make_async_copy(
                fourier_ref.at[:, points], fourier.at[:, points], fetched.at[k]
            )
        )
        fetches[k].start()
    for source in range(LAT_PARTS):
        wide[source * PITCH : source * PITCH + PAIRS * ROWS, :] = (
            grid_ref[source].astype(jnp.float32).reshape(PAIRS * ROWS, LANES)
        )
    is_south = lax.axis_index("lat") >= LAT_PARTS // 2

    def transpose(first, count, row, group):
        source_row = jnp.where(is_south, ROWS - 1 - (first + row), first + row)
        stacked = jnp.concatenate(
            [
                wide[pl.ds((2 * group + t) * ROWS + source_row, LAT_PARTS, stride=PITCH), :]
                for t in range(2)
            ],
            axis=0,
        ).T
        for q in range(4):
            turned[
                4 * group + q, pl.ds(OWN_FIELDS * first + row, OWN_FIELDS, stride=count), :
            ] = stacked[q * OWN_FIELDS : (q + 1) * OWN_FIELDS]

    def narrow(first, count, q):
        rows = slice(OWN_FIELDS * first, OWN_FIELDS * (first + count))
        left[rows, q * LANES : (q + 1) * LANES] = turned[q, rows, :].astype(jnp.bfloat16)

    def preparation(first, count):
        steps = []
        for group in range(2):
            steps += [
                functools.partial(transpose, first, count, row, group) for row in range(count)
            ]
            steps += [functools.partial(narrow, first, count, 4 * group + q) for q in range(4)]
        return steps

    copies = []
    for step in preparation(*BANDS[0]):
        step()
    for band, (first, count) in enumerate(BANDS):
        rows = slice(OWN_FIELDS * first, OWN_FIELDS * (first + count))
        pending = preparation(*BANDS[band + 1]) if band + 1 < len(BANDS) else []
        share = -(-len(pending) // (NLON // WIDTH))
        for k in range(NLON // WIDTH):
            points = slice(k * WIDTH, (k + 1) * WIDTH)
            if band == 0:
                fetches[k].wait()
            product = jnp.dot(left[rows, :], fourier[:, points], preferred_element_type=jnp.float32)
            done[:, first : first + count, points] = product.reshape(OWN_FIELDS, count, WIDTH)
            copy = pltpu.make_async_copy(
                done.at[:, first : first + count, points],
                out_ref.at[:, first : first + count, points],
                arrived.at[len(copies)],
            )
            copy.start()
            copies.append(copy)
            for step in pending[k * share : (k + 1) * share]:
                step()
    for copy in copies:
        copy.wait()


def synthesize(grid_spec, fourier):
    return pl.pallas_call(
        synthesis_kernel,
        in_specs=[whole, outside],
        out_specs=outside,
        out_shape=jax.ShapeDtypeStruct((OWN_FIELDS, ROWS, NLON), jnp.float32),
        scratch_shapes=[
            pltpu.VMEM((LAT_PARTS * PITCH, LANES), jnp.float32),
            pltpu.VMEM((8, OWN_FIELDS * ROWS, LANES), jnp.float32),
            pltpu.VMEM((OWN_FIELDS * ROWS, 2 * M), jnp.bfloat16),
            pltpu.VMEM((OWN_FIELDS, ROWS, NLON), jnp.float32),
            pltpu.VMEM((2 * M, NLON), jnp.bfloat16),
            pltpu.SemaphoreType.DMA((len(BANDS) * (NLON // WIDTH),)),
            pltpu.SemaphoreType.DMA((NLON // WIDTH,)),
        ],
        compiler_params=vmem_params(52),
        name="synthesis",
    )(grid_spec, fourier)


def exchanged(spectra):
    received = [spectra[0]]
    for offset in range(1, SCALE_PARTS):
        pairs = [(k, partner(k, offset)) for k in range(SCALE_PARTS)]
        received.append(lax.ppermute(spectra[offset], "scale", pairs))
    return received


def on_device(state, noise, slot_wavenumber, timescale, lengthscale):
    lats = jnp.asarray(latitude_constants())
    head = jnp.asarray(log_head_table())
    new_state, *spectra = update(timescale[None], lengthscale[None], state, noise)
    spectra = exchanged(spectra)
    table = legendre_table(slot_wavenumber, lats, head)
    grid_spec = project(slot_wavenumber, spectra, table)
    grid_spec = lax.all_to_all(grid_spec, "lat", 0, 0, tiled=True)
    pattern = synthesize(grid_spec, fourier_table(slot_wavenumber))
    return (new_state, pattern)


def solution(mesh):
    placed = (P("lat", None, None, "scale"), P("lat", None, None, "scale"), P(), P(), P())
    return jax.shard_map(
        on_device,
        mesh=mesh,
        in_specs=placed,
        out_specs=(P("lat", None, None, "scale"), P("scale", "lat", None)),
        check_vma=False,
    )
```
